32 devices in a mesh: expert: 4 (over y, core), tensor: 8 (over z, x).
Axes of the slice: x: 2, y: 2, z: 4, core: 2. Of those that a mesh axis runs over, the one named last changes fastest.
Arguments:
- tokens: bfloat16 [1024, 6144], P('expert'), may hold values from -6 to 6
- expert_ids: int32 [1024, 2], P('expert'), may hold values from 0 to 3, all different within a row; in each aligned block of 256 rows (0 to 255, 256 to 511, ...) at most 192 rows name the same one
- gate_weights: float32 [1024, 2], P('expert'), may hold values from 0.2 to 1
- w_gate: bfloat16 [4, 6144, 16384], P('expert', None, 'tensor'), may hold values from -0.078125 to 0.078125
- w_up: bfloat16 [4, 6144, 16384], P('expert', None, 'tensor'), may hold values from -0.078125 to 0.078125
- w_down: bfloat16 [4, 16384, 6144], P('expert', 'tensor'), may hold values from -0.0625 to 0.0625
Outputs:
- mixed: bfloat16 [1024, 6144], P(('expert', 'tensor'))
The draws below stay inside these ranges and needn't reach their ends.
Inputs may be any that keep to these rules, and one draw needn't show every extreme that they name: `expert_ids`: each token names two different experts. Among the 256 tokens held at one index along `expert`, no expert is named by more than 192 tokens, and in some such blocks one expert is named by exactly 192.
All inputs are finite; a program needn't handle non-finite values.
Results may differ from the reference program's by a relative error of at most 0.005.
Values may be sent and summed in bfloat16 or wider, within the bound.
A program may use at most 192 MiB of HBM per device.

```python
import math
import jax
import jax.numpy as jnp
import numpy as np
from jax import lax

D = 6144
FF = 16384
EXPERTS = 4
TOK_DEV = 256
CAP = 192
TOKENS = 1024


def with_spikes(entries, key, source, target, blocks, factor):
    owner, partner = [(jnp.arange(entries.shape[position]) // (entries.shape[position] // blocks)).reshape([-1 if axis == position else 1 for axis in range(entries.ndim)]) for position in (source, target)]
    chosen = jax.random.permutation(key, blocks)[partner]
    strong = (owner == chosen) | (owner == (partner + blocks // 2) % blocks)
    return jnp.where(strong, factor * entries, entries)


def block_scale(rng, dims, pieces, low, top_value):
    def one(position, parts):
        steps = jax.random.uniform(jax.random.fold_in(jax.random.fold_in(rng, 6), position), (parts,), jnp.float32, low / len(pieces), top_value / len(pieces))
        return jnp.repeat(jnp.exp(steps), dims[position] // parts).reshape((-1,) + (1,) * (len(dims) - position - 1))

    level = one(*pieces[0])
    for cut in pieces[1:]:
        level = level * one(*cut)
    return level


def routed_block(rng, own, number, rows, amount, top, most, skew):
    ranking = jax.random.permutation(rng, amount)
    packed, common = portions_of(amount, rows * top, most, skew, True), portions_of(amount, rows * top, most, skew, False)
    places = jnp.arange(amount)

    def named(sizes, offset_by):
        used = int((sizes > 0).sum())
        fixed = max(1, used // 4)
        moved = fixed + (places - fixed + offset_by * (used - fixed)) % max(1, amount - fixed)
        return jnp.zeros((amount,), jnp.int32).at[ranking[jnp.where(places < fixed, places, moved)]].set(jnp.asarray(sizes, jnp.int32))

    sizes = jnp.where(number % 4 == 0, named(packed, number // 4), named(common, number - number // 4 - 1))
    mixed = jax.random.permutation(jax.random.fold_in(own, 3), amount)
    source_of, sink = mixed[0:amount // 2 * 2:2], mixed[1:amount // 2 * 2:2]
    slack = jnp.minimum(sizes[source_of] - 1, most - sizes[sink]) // 2
    slack = jnp.where((source_of == ranking[0]) | (sink == ranking[0]) | (sizes[sink] == 0), 0, jnp.maximum(slack, 0))
    moved = jax.random.randint(jax.random.fold_in(own, 4), (amount // 2,), 0, 1 << 20) % (slack + 1)
    sizes = sizes.at[source_of].add(-moved).at[sink].add(moved)
    items = jnp.searchsorted(jnp.cumsum(sizes), jnp.arange(rows * top), side="right").astype(jnp.int32)
    grid = items.reshape(top, rows).T
    grid = grid[jax.random.permutation(jax.random.fold_in(own, 1), rows)]
    offset_by = jax.random.randint(jax.random.fold_in(own, 2), (rows, 1), 0, top)
    return jnp.take_along_axis(grid, (jnp.arange(top)[None, :] + offset_by) % top, axis=1)


def portions_of(number_of, total, limit, skew, full):
    weights = [(1 << 20) // math.isqrt(grade ** skew) + 1 for grade in range(1, number_of + 1)]
    largest = limit if full else min(limit, max(-(-total // number_of), total * weights[0] // sum(weights)))
    least = 1 if total - largest >= number_of - 1 else 0
    counts, spare = [largest] + [least] * (number_of - 1), total - largest - least * (number_of - 1)
    while spare > 0:
        movable = [i for i in range(1, number_of) if counts[i] < largest] or [i for i in range(1, number_of) if counts[i] < limit]
        whole, budget = sum([weights[i] for i in movable]), spare
        for i in movable:
            more = min(limit - counts[i], max(1, budget * weights[i] // whole), spare)
            counts[i] = counts[i] + more
            spare = spare - more
    return np.array(counts)


def noise(stream_key, shape, deviation, most, pieces=(), held_as=jnp.bfloat16):
    entries = deviation * jax.random.normal(stream_key, shape, jnp.float32)
    if pieces:
        entries = entries * block_scale(stream_key, shape, pieces, -0.22, 0.18)
    return jnp.clip(entries, -most, most).astype(held_as)


def gaussian_with(key, dims, deviation, limit, cuts, heavy, dtype=jnp.bfloat16):
    values = deviation * jax.random.normal(key, dims, jnp.float32)
    if cuts:
        values = values * block_scale(key, dims, cuts, -0.22, 0.18)
    return jnp.clip(with_spikes(values, jax.random.fold_in(key, 3), *heavy), -limit, limit).astype(dtype)


def setup_inputs(seed: int = 0) -> dict:
    streams_of = jax.random.split(jax.random.key(seed), 7)
    tokens = noise(streams_of[0], (TOKENS, D), 1.0, 6.0, ((0, 4),))
    expert_ids_keys = jax.random.split(jax.random.fold_in(streams_of[1], 1), TOKENS // TOK_DEV)
    expert_ids_turns = jax.random.permutation(jax.random.fold_in(streams_of[1], 3), TOKENS // TOK_DEV)
    expert_ids = jax.vmap(lambda own, number: routed_block(jax.random.fold_in(streams_of[1], 2), own, number, TOK_DEV, EXPERTS, 2, CAP, 2))(expert_ids_keys, expert_ids_turns).reshape((TOKENS, 2))
    gate_weights = jnp.clip(0.2 + 0.8 * jax.random.uniform(streams_of[2], (TOKENS, 2), jnp.float32) ** block_scale(streams_of[2], (TOKENS, 2), ((0, 4),), -0.2, 0.2), 0.2, 1.0)
    w_gate = noise(streams_of[3], (EXPERTS, D, FF), D ** -0.5, 0.078125, ((0, 4), (2, 8)))
    w_up = noise(streams_of[4], (EXPERTS, D, FF), D ** -0.5, 0.078125, ((0, 4), (2, 8)))
    w_down = gaussian_with(streams_of[5], (EXPERTS, FF, D), FF ** -0.5, 0.0625, ((0, 4), (1, 8)), (1, 2, 8, 2.0))
    return dict(tokens=tokens, expert_ids=expert_ids, gate_weights=gate_weights, w_gate=w_gate, w_up=w_up, w_down=w_down)


def reference(tokens, expert_ids, gate_weights, w_gate, w_up, w_down):
    def add_expert(expert, total):
        gate_proj = jnp.dot(tokens, w_gate[expert], preferred_element_type=jnp.float32)
        up_proj = jnp.dot(tokens, w_up[expert], preferred_element_type=jnp.float32)
        hidden = (jax.nn.silu(gate_proj) * up_proj).astype(jnp.bfloat16)
        output = jnp.dot(hidden, w_down[expert], preferred_element_type=jnp.float32)
        weight = jnp.sum(jnp.where(expert_ids == expert, gate_weights, jnp.zeros_like(gate_weights)), axis=1)
        return total + output * weight[:, None]

    total = lax.fori_loop(0, EXPERTS, add_expert, jnp.zeros((TOKENS, D), jnp.float32))
    return total.astype(jnp.bfloat16)
```

```python
import functools

import jax
import jax.numpy as jnp
from jax import lax
from jax.experimental import pallas as pl
from jax.experimental.pallas import tpu as pltpu
from jax.sharding import PartitionSpec as P

MESH = pl.DeviceIdType.MESH
F32, BF16 = jnp.float32, jnp.bfloat16


def plan(events, ends):
    table = [[] for _ in range(len(ends) + 1)]
    for when, action in sorted(events, key=lambda item: item[0]):
        step = next((i for i, end in enumerate(ends) if end >= when), len(ends))
        table[step].append(action)
    return table


def moe_kernel(
    cfg,
    tok_hbm, wts, wg_hbm, wu_hbm, wd_hbm,
    out_ref,
    raw, xc, hid, wgu, wdn, keep, give, d2d_in, x_in, z_in, y_in, acc, rt, emat, wcol,
    s_tok, s_gu, s_dn, s_rt, s_pt, s_yp, s_zp, s_fy, s_fz, s_d2d, s_x, s_z, s_y,
):
    experts, parts, rows, cap, width, ff = cfg["dims"]
    ft, cw, pieces, slots = cfg["ft"], cfg["cw"], cfg["pieces"], cfg["slots"]
    pairs, nz, owned = experts // 2, parts // 2, rows // parts
    nch, nf, half = width // cw, ff // ft, rows // 2
    prow = half // pieces

    e = lax.axis_index("expert")
    t = lax.axis_index("tensor")
    yy, core = e // 2, e % 2
    z, x = t // 2, t % 2
    mate = e + 1 - 2 * core
    xmate = t + 1 - 2 * x
    z0 = z % 2
    zmate = t + 2 - 4 * z0

    def pair_dev(k):
        return ((yy + k + pairs) % pairs) * 2 + core

    def remote(src, dst, sems, index, dev):
        return pltpu.make_async_remote_copy(
            src_ref=src, dst_ref=dst, send_sem=sems.at[(0,) + index], recv_sem=sems.at[(1,) + index],
            device_id=dev, device_id_type=MESH)

    def route_copy(k):
        peer = (e + k) % experts
        return remote(wts.at[peer], rt.at[e], s_rt, (k - 1,), (peer, t))

    def mate_tokens():
        return remote(tok_hbm, raw.at[0, 1], s_pt, (), (mate, t))

    def piece_rows(which, p):
        return pl.ds(pl.multiple_of(which * half + p * prow, prow), prow)

    def y_piece(q, p):
        part = piece_rows(z0, p)
        return remote(tok_hbm.at[part], raw.at[q, 0, part], s_yp, (q - 1, p), (pair_dev(-q), t))

    def z_piece(q, p):
        part = piece_rows(z0, p)
        return remote(raw.at[q, 0, part], raw.at[q, 0, part], s_zp, (q - 1, p), (e, zmate))

    def fwd_y(q, p):
        part = piece_rows(z0, p)
        return remote(raw.at[q, 0, part], raw.at[q, 1, part], s_fy, (q - 1, p), (mate, t))

    def fwd_z(q, p):
        part = piece_rows(1 - z0, p)
        return remote(raw.at[q, 0, part], raw.at[q, 1, part], s_fz, (q - 1, p), (mate, t))

    def d2d(q, c):
        return remote(give.at[c], d2d_in.at[q, c], s_d2d, (q, c), (mate, t))

    def xsend(q, c):
        return remote(keep.at[q, c, :, 1 - x], x_in.at[q, c], s_x, (q, c), (e, xmate))

    def zsend(q, c, k):
        to = (z + k) % nz
        return remote(keep.at[q, c, to, x], z_in.at[q, c, k - 1], s_z, (q, c), (e, to * 2 + x))

    def zall(q, c):
        return remote(z_in.at[q, c], z_in.at[q, c], s_z, (q, c), (e, xmate))

    def ysend(q, c):
        return remote(keep.at[q, c, z, x], y_in.at[q - 1, c], s_y, (q - 1, c), (pair_dev(q), t))

    def gu_load(j, slot):
        cols = pl.ds(pl.multiple_of(j * ft, ft), ft)
        return [pltpu.make_async_copy(src.at[:, cols], wgu.at[slot, i], s_gu.at[slot, i])
                for i, src in enumerate((wg_hbm, wu_hbm))]

    def dn_load(c, slot):
        cols = pl.ds(pl.multiple_of(c * cw, cw), cw)
        return pltpu.make_async_copy(wd_hbm.at[:, cols], wdn.at[slot], s_dn.at[slot])

    def stage_mate(q, c):
        d2d(q, c).wait_recv()
        keep[q, c] = (keep[q, c].astype(F32) + d2d_in[q, c].astype(F32)).astype(BF16)
        xsend(q, c).start()

    def stage_x(q, c):
        xsend(q, c).wait_recv()
        total = keep[q, c, :, x].astype(F32) + x_in[q, c].astype(F32)
        keep[q, c, :, x] = total.astype(BF16)
        for k in range(1, nz):
            zsend(q, c, k).start()

    def stage_z(q, c):
        zall(q, c).wait_recv()
        total = keep[q, c, z, x].astype(F32)
        for k in range(1, nz):
            total += z_in[q, c, k - 1].astype(F32)
        if q == 0:
            acc[c] = total
        else:
            zall(q, c).wait_send()
            keep[q, c, z, x] = total.astype(BF16)
            ysend(q, c).start()

    def stage_y(c):
        total = acc[c]
        for q in range(1, pairs):
            ysend(q, c).wait_recv()
            total += y_in[q - 1, c].astype(F32)
        out_ref[:, pl.ds(pl.multiple_of(c * cw, cw), cw)] = total.astype(out_ref.dtype)

    own_tok = pltpu.make_async_copy(tok_hbm, raw.at[0, 0], s_tok)
    own_tok.start()
    for slot in range(2):
        for copy in gu_load(slot % nf, slot):
            copy.start()
    for slot in range(slots):
        dn_load(slot % nch, slot).start()

    barrier = pltpu.get_barrier_semaphore()
    peers = [((e + k) % experts, t) for k in range(1, experts)] + [(e, xmate)]
    peers += [(e, ((z + k) % nz) * 2 + x) for k in range(1, nz)]
    for peer in peers:
        pl.semaphore_signal(barrier, inc=1, device_id=peer, device_id_type=MESH)
    pl.semaphore_wait(barrier, len(peers))

    mate_tokens().start()
    for k in range(1, experts):
        route_copy(k).start()
    for p in range(pieces):
        for q in range(1, pairs):
            y_piece(q, p).start()
    rt[e] = wts[e]
    for k in range(1, experts):
        back = (e + experts - k) % experts
        remote(wts.at[back], rt.at[back], s_rt, (k - 1,), (back, t)).wait_recv()

    def compact(q, slot):
        block = ((yy + q) % pairs) * 2 + (core if slot == 0 else 1 - core)
        w = rt[block]
        mask = jnp.where(w > 0, 1.0, 0.0).astype(BF16)
        upto = lax.broadcasted_iota(jnp.int32, (rows, rows), 0)
        here = lax.broadcasted_iota(jnp.int32, (rows, rows), 1)
        before = jnp.where(upto <= here, 1.0, 0.0).astype(BF16)
        place = jnp.dot(mask, before, preferred_element_type=F32)
        place = jnp.where(w > 0, place - 1.0, -1.0)[:1]
        lane = lax.broadcasted_iota(jnp.int32, (cap, rows), 0).astype(F32)
        pick = jnp.broadcast_to(place, (cap, rows)) == lane
        wcol[slot] = jnp.broadcast_to(
            jnp.sum(jnp.where(pick, jnp.broadcast_to(w[:1], (cap, rows)), 0.0), axis=1, keepdims=True), (cap, 128))
        pick = jnp.where(pick, 1.0, 0.0).astype(BF16)
        after = jnp.where(here <= upto, 1.0, 0.0).astype(BF16)
        same = jnp.where(here == upto, 1.0, 0.0).astype(BF16)
        nt = (((1,), (1,)), ((), ()))
        place_col = lax.dot_general(after, mask, nt, preferred_element_type=F32)[:, :1]
        mask_col = lax.dot_general(same, mask, nt, preferred_element_type=F32)[:, :1]
        place_col = jnp.where(mask_col > 0.5, place_col - 1.0, -1.0)
        column = lax.broadcasted_iota(jnp.int32, (rows, cap), 1).astype(F32)
        emat[slot] = jnp.where(jnp.broadcast_to(place_col, (rows, cap)) == column, 1.0, 0.0).astype(BF16)

        if q == 0 and slot == 0:
            own_tok.wait()
        elif q == 0:
            mate_tokens().wait_recv()
        elif slot == 1:
            for p in range(pieces):
                fwd_y(q, p).wait_recv()
                fwd_z(q, p).wait_recv()

        @pl.loop(0, nch)
        def _(c):
            cols = pl.ds(pl.multiple_of(c * cw, cw), cw)
            got = jnp.dot(pick, raw[q, slot, :, cols], preferred_element_type=F32)
            xc[slot * cap:(slot + 1) * cap, cols] = got.astype(BF16)

    gu_t, per_x = cfg["gu_t"], cfg["per_x"]
    pass_t = nf * gu_t + nch
    gu_end = [(j + 1) * gu_t for j in range(nf)]
    dn_end = [nf * gu_t + j + 1 for j in range(nch)]

    def gather_events(q):
        events = []
        for p in range(pieces):
            arrive = cfg["y0"] + cfg["y_t"] * (p + 1)

            def one(p=p):
                y_piece(q, p).wait_recv()
                z_piece(q, p).start()
                fwd_y(q, p).start()

            def two(p=p):
                z_piece(q, p).wait_recv()
                fwd_z(q, p).start()

            events.append((arrive, one))
            events.append((arrive + cfg["y_t"] + cfg["hop"] + 0.5 * gu_t, two))
        return events

    def run(actions):
        for action in actions:
            action()

    for q in range(pairs):
        events = []
        if q == 0:
            for k in range(1, pairs):
                events += gather_events(k)
        else:
            start = -nch - cfg["lag"]
            for c in range(nch):
                at = start + cfg["hop"] + per_x * (c + 1)
                events.append((at, functools.partial(stage_x, q - 1, c)))
                events.append((max(at + cfg["z_t"], nf * gu_t + c + 0.5), functools.partial(stage_z, q - 1, c)))
        for c in range(nch):
            events.append((nf * gu_t + c + 2.5, functools.partial(stage_mate, q, c)))
        table = plan(events, gu_end + dn_end)

        for slot in range(2):
            compact(q, slot)

        @pl.loop(0, nf)
        def _(j):
            slot = j % 2
            for copy in gu_load(j, slot):
                copy.wait()
            gate = jnp.dot(xc[...], wgu[slot, 0], preferred_element_type=F32)
            up = jnp.dot(xc[...], wgu[slot, 1], preferred_element_type=F32)
            hid[:, pl.ds(pl.multiple_of(j * ft, ft), ft)] = (gate * (1.0 / (1.0 + jnp.exp(-gate))) * up).astype(BF16)

            @pl.when(j + 2 < nf)
            def _():
                for copy in gu_load(j + 2, slot):
                    copy.start()

            for step in range(nf):
                if table[step]:
                    pl.when(j == step)(functools.partial(run, table[step]))

        if q + 1 < pairs:
            for slot in range(2):
                for copy in gu_load(slot % nf, slot):
                    copy.start()

        @pl.loop(0, nch)
        def _(c):
            slot = c % slots
            dn_load(c, slot).wait()
            y = jnp.dot(hid[...], wdn[slot], preferred_element_type=F32)
            y0 = (y[:cap] * wcol[0, :, :1]).astype(BF16)
            y1 = (y[cap:] * wcol[1, :, :1]).astype(BF16)
            if q > 0:
                d2d(q - 1, c).wait_send()
            give[c] = jnp.dot(emat[1], y1, preferred_element_type=F32).astype(BF16).reshape(nz, 2, owned, cw)
            d2d(q, c).start()
            keep[q, c] = jnp.dot(emat[0], y0, preferred_element_type=F32).astype(BF16).reshape(nz, 2, owned, cw)

            ahead = c + slots
            if q + 1 < pairs:
                dn_load(ahead % nch, slot).start()
            else:
                @pl.when(ahead < nch)
                def _():
                    dn_load(ahead, slot).start()

            for step in range(nch):
                if table[nf + step]:
                    pl.when(c == step)(functools.partial(run, table[nf + step]))

        run(table[nf + nch])

    last = pairs - 1

    @pl.loop(0, nch + 4)
    def _(n):
        @pl.when(n < nch)
        def _():
            stage_x(last, n)

        @pl.when((n >= 2) & (n < nch + 2))
        def _():
            stage_z(last, n - 2)

        @pl.when(n >= 4)
        def _():
            stage_y(n - 4)

    mate_tokens().wait_send()
    for k in range(1, experts):
        route_copy(k).wait_send()
    for q in range(1, pairs):
        for p in range(pieces):
            for copy in (y_piece, z_piece, fwd_y, fwd_z):
                copy(q, p).wait_send()

    @pl.loop(0, nch)
    def _(c):
        d2d(last, c).wait_send()
        for q in range(pairs):
            xsend(q, c).wait_send()
            if q == 0:
                zall(q, c).wait_send()
            else:
                ysend(q, c).wait_send()


def body(tokens, expert_ids, gate_weights, w_gate, w_up, w_down):
    rows, width = tokens.shape
    experts = lax.axis_size("expert")
    parts = lax.axis_size("tensor")
    ff = w_gate.shape[2]
    cap = rows * 3 // 4
    pairs, nz, owned = experts // 2, parts // 2, rows // parts
    ft, cw, pieces, slots = 256, 512, 8, 3
    nch = width // cw
    others = pairs - 1

    hot = expert_ids[None, :, :] == jnp.arange(experts, dtype=jnp.int32)[:, None, None]
    weight = jnp.sum(jnp.where(hot, gate_weights[None], 0.0), axis=2)
    weight = jnp.broadcast_to(weight[:, None, :], (experts, 8, rows))

    cfg = dict(
        dims=(experts, parts, rows, cap, width, ff), ft=ft, cw=cw, pieces=pieces, slots=slots,
        gu_t=2.75, per_x=3.0, y0=-2.0, y_t=4.5, hop=2.0, lag=4.0, z_t=6.0,
    )
    dma = pltpu.SemaphoreType.DMA
    any_space = pl.BlockSpec(memory_space=pl.ANY)
    vmem = pl.BlockSpec(memory_space=pltpu.VMEM)
    return pl.pallas_call(
        functools.partial(moe_kernel, cfg),
        out_shape=jax.ShapeDtypeStruct((owned, width), BF16),
        in_specs=[any_space, vmem, any_space, any_space, any_space],
        out_specs=vmem,
        scratch_shapes=[
            pltpu.VMEM((pairs, 2, rows, width), BF16),
            pltpu.VMEM((2 * cap, width), BF16),
            pltpu.VMEM((2 * cap, ff), BF16),
            pltpu.VMEM((2, 2, width, ft), BF16),
            pltpu.VMEM((slots, ff, cw), BF16),
            pltpu.VMEM((pairs, nch, nz, 2, owned, cw), BF16),
            pltpu.VMEM((nch, nz, 2, owned, cw), BF16),
            pltpu.VMEM((pairs, nch, nz, 2, owned, cw), BF16),
            pltpu.VMEM((pairs, nch, nz, owned, cw), BF16),
            pltpu.VMEM((pairs, nch, nz - 1, owned, cw), BF16),
            pltpu.VMEM((others, nch, owned, cw), BF16),
            pltpu.VMEM((nch, owned, cw), F32),
            pltpu.VMEM((experts, 8, rows), F32),
            pltpu.VMEM((2, rows, cap), BF16),
            pltpu.VMEM((2, cap, 128), F32),
            dma,
            dma((2, 2)),
            dma((slots,)),
            dma((2, experts - 1)),
            dma((2,)),
            dma((2, others, pieces)),
            dma((2, others, pieces)),
            dma((2, others, pieces)),
            dma((2, others, pieces)),
            dma((2, pairs, nch)),
            dma((2, pairs, nch)),
            dma((2, pairs, nch)),
            dma((2, others, nch)),
        ],
        compiler_params=pltpu.CompilerParams(
            collective_id=0, has_side_effects=True, vmem_limit_bytes=67043328),
    )(tokens, weight, w_gate[0], w_up[0], w_down[0])


def solution(mesh):
    placed = (
        P("expert", None),
        P("expert", None),
        P("expert", None),
        P("expert", None, "tensor"),
        P("expert", None, "tensor"),
        P("expert", "tensor", None),
    )
    return jax.shard_map(
        body, mesh=mesh, in_specs=placed, out_specs=P(("expert", "tensor"), None), check_vma=False
    )
```

```python
import functools

import jax
import jax.numpy as jnp
from jax import lax
from jax.experimental import pallas as pl
from jax.experimental.pallas import tpu as pltpu
from jax.sharding import PartitionSpec as P

MESH = pl.DeviceIdType.MESH
F32, BF16 = jnp.float32, jnp.bfloat16


def plan(events, ends):
    table = [[] for _ in range(len(ends) + 1)]
    for when, action in sorted(events, key=lambda item: item[0]):
        step = next((i for i, end in enumerate(ends) if end >= when), len(ends))
        table[step].append(action)
    return table


def moe_kernel(
    cfg,
    tok_hbm, wts, wg_hbm, wu_hbm, wd_hbm,
    out_ref,
    raw, xc, hid, wgu, wdn, ys, keep, give, d2d_in, x_in, za_in, z_in, y_in, acc, rt, emat, wcol,
    s_tok, s_gu, s_dn, s_rt, s_pt, s_yp, s_xp, s_zp, s_dg, s_fw, s_d2d, s_x, s_za, s_z, s_y,
):
    experts, parts, rows, cap, width, ff = cfg["dims"]
    ft, cw, pieces, slots = cfg["ft"], cfg["cw"], cfg["pieces"], cfg["slots"]
    pairs, nz, owned = experts // 2, parts // 2, rows // parts
    nch, nf, quarter = width // cw, ff // ft, rows // 4
    prow = quarter // pieces

    e = lax.axis_index("expert")
    t = lax.axis_index("tensor")
    yy, core = e // 2, e % 2
    z, x = t // 2, t % 2
    mate = e + 1 - 2 * core
    xmate = t + 1 - 2 * x
    z0 = z % 2
    zmate = t + 2 - 4 * z0
    z1, nz1 = z // 2, nz // 2

    def pair_dev(k):
        return ((yy + k + pairs) % pairs) * 2 + core

    def remote(src, dst, sems, index, dev):
        return pltpu.make_async_remote_copy(
            src_ref=src, dst_ref=dst, send_sem=sems.at[(0,) + index], recv_sem=sems.at[(1,) + index],
            device_id=dev, device_id_type=MESH)

    def route_copy(k):
        peer = (e + k) % experts
        return remote(wts.at[peer], rt.at[e], s_rt, (k - 1,), (peer, t))

    def mate_tokens():
        return remote(tok_hbm, raw.at[0, 1], s_pt, (), (mate, t))

    quarters = (2 * z0 + x, 2 * z0 + 1 - x, 2 * (1 - z0) + x, 2 * (1 - z0) + 1 - x)

    def piece_rows(kind, p):
        return pl.ds(pl.multiple_of(quarters[kind] * quarter + p * prow, prow), prow)

    def y_piece(q, p):
        part = piece_rows(0, p)
        return remote(tok_hbm.at[part], raw.at[q, 0, part], s_yp, (q - 1, p), (pair_dev(-q), t))

    def along(q, part, sems, p, dev):
        return remote(raw.at[q, 0, part], raw.at[q, 0, part], sems, (q - 1, p), dev)

    def x_piece(q, p):
        return along(q, piece_rows(0, p), s_xp, p, (e, xmate))

    def z_piece(q, p):
        return along(q, piece_rows(0, p), s_zp, p, (e, zmate))

    def diagonal(q, p):
        if p % 2 == 0:
            return along(q, piece_rows(2, p), s_dg, p, (e, xmate))
        return along(q, piece_rows(1, p), s_dg, p, (e, zmate))

    def forward(q, kind, p):
        part = piece_rows(kind, p)
        return remote(raw.at[q, 0, part], raw.at[q, 1, part], s_fw, (q - 1, kind * pieces + p), (mate, t))

    def d2d(q, c):
        return remote(give.at[c], d2d_in.at[q, c], s_d2d, (q, c), (mate, t))

    def xsend(q, c):
        return remote(keep.at[q, c, :, :, 1 - x], x_in.at[q, c], s_x, (q, c), (e, xmate))

    def zswap(q, c):
        return remote(keep.at[q, c, :, 1 - z0, x], za_in.at[q, c], s_za, (q, c), (e, zmate))

    def zsend(q, c, k):
        to = (z1 + k) % nz1
        return remote(keep.at[q, c, to, z0, x], z_in.at[q, c, k - 1], s_z, (q, c), (e, (to * 2 + z0) * 2 + x))

    def zall(q, c):
        return remote(z_in.at[q, c], z_in.at[q, c], s_z, (q, c), (e, xmate))

    def ysend(q, c):
        return remote(keep.at[q, c, z1, z0, x], y_in.at[q - 1, c], s_y, (q - 1, c), (pair_dev(q), t))

    def gu_load(j, slot):
        cols = pl.ds(pl.multiple_of(j * ft, ft), ft)
        return [pltpu.make_async_copy(src.at[:, cols], wgu.at[slot, i], s_gu.at[slot, i])
                for i, src in enumerate((wg_hbm, wu_hbm))]

    def dn_load(c, slot):
        cols = pl.ds(pl.multiple_of(c * cw, cw), cw)
        return pltpu.make_async_copy(wd_hbm.at[:, cols], wdn.at[slot], s_dn.at[slot])

    def stage_mate(q, c):
        d2d(q, c).wait_recv()
        keep[q, c] = (keep[q, c].astype(F32) + d2d_in[q, c].astype(F32)).astype(BF16)
        xsend(q, c).start()

    def stage_x(q, c):
        xsend(q, c).wait_recv()
        total = keep[q, c, :, :, x].astype(F32) + x_in[q, c].astype(F32)
        keep[q, c, :, :, x] = total.astype(BF16)
        zswap(q, c).start()

    def stage_swap(q, c):
        zswap(q, c).wait_recv()
        total = keep[q, c, :, z0, x].astype(F32) + za_in[q, c].astype(F32)
        keep[q, c, :, z0, x] = total.astype(BF16)
        for k in range(1, nz1):
            zsend(q, c, k).start()

    def stage_z(q, c):
        zall(q, c).wait_recv()
        total = keep[q, c, z1, z0, x].astype(F32)
        for k in range(1, nz1):
            total += z_in[q, c, k - 1].astype(F32)
        if q == 0:
            acc[c] = total
        else:
            zall(q, c).wait_send()
            keep[q, c, z1, z0, x] = total.astype(BF16)
            ysend(q, c).start()

    def stage_y(c):
        total = acc[c]
        for q in range(1, pairs):
            ysend(q, c).wait_recv()
            total += y_in[q - 1, c].astype(F32)
        out_ref[:, pl.ds(pl.multiple_of(c * cw, cw), cw)] = total.astype(out_ref.dtype)

    own_tok = pltpu.make_async_copy(tok_hbm, raw.at[0, 0], s_tok)
    own_tok.start()
    for copy in gu_load(0, 0):
        copy.start()
    rt[e] = wts[e]
    barrier = pltpu.get_barrier_semaphore()
    peers = [((e + k) % experts, t) for k in range(1, experts)] + [(e, xmate)]
    peers += [(e, ((z + k) % nz) * 2 + x) for k in range(1, nz)]
    for peer in peers:
        pl.semaphore_signal(barrier, inc=1, device_id=peer, device_id_type=MESH)

    def greet():
        pl.semaphore_wait(barrier, len(peers))
        for k in range(1, experts):
            route_copy(k).start()
        mate_tokens().start()
        for p in range(pieces):
            for q in range(1, pairs):
                y_piece(q, p).start()
        for slot in range(slots):
            dn_load(slot % nch, slot).start()

    def routes():
        for k in range(1, experts):
            back = (e + experts - k) % experts
            remote(wts.at[back], rt.at[back], s_rt, (k - 1,), (back, t)).wait_recv()

    def compact(q, slot):
        block = ((yy + q) % pairs) * 2 + (core if slot == 0 else 1 - core)
        w = rt[block]
        mask = jnp.where(w > 0, 1.0, 0.0).astype(BF16)
        upto = lax.broadcasted_iota(jnp.int32, (rows, rows), 0)
        here = lax.broadcasted_iota(jnp.int32, (rows, rows), 1)
        before = jnp.where(upto <= here, 1.0, 0.0).astype(BF16)
        place = jnp.dot(mask, before, preferred_element_type=F32)
        place = jnp.where(w > 0, place - 1.0, -1.0)[:1]
        lane = lax.broadcasted_iota(jnp.int32, (cap, rows), 0).astype(F32)
        pick = jnp.broadcast_to(place, (cap, rows)) == lane
        wcol[slot] = jnp.broadcast_to(
            jnp.sum(jnp.where(pick, jnp.broadcast_to(w[:1], (cap, rows)), 0.0), axis=1, keepdims=True), (cap, 128))
        pick = jnp.where(pick, 1.0, 0.0).astype(BF16)
        after = jnp.where(here <= upto, 1.0, 0.0).astype(BF16)
        same = jnp.where(here == upto, 1.0, 0.0).astype(BF16)
        nt = (((1,), (1,)), ((), ()))
        place_col = lax.dot_general(after, mask, nt, preferred_element_type=F32)[:, :1]
        mask_col = lax.dot_general(same, mask, nt, preferred_element_type=F32)[:, :1]
        place_col = jnp.where(mask_col > 0.5, place_col - 1.0, -1.0)
        column = lax.broadcasted_iota(jnp.int32, (rows, cap), 1).astype(F32)
        emat[slot] = jnp.where(jnp.broadcast_to(place_col, (rows, cap)) == column, 1.0, 0.0).astype(BF16)

        if q == 0 and slot == 0:
            own_tok.wait()
        elif q == 0:
            mate_tokens().wait_recv()
        elif slot == 1:
            for p in range(pieces):
                for kind in range(4):
                    forward(q, kind, p).wait_recv()

        wide = 4 * cw if nch % 4 == 0 else cw

        @pl.loop(0, width // wide)
        def _(c):
            cols = pl.ds(pl.multiple_of(c * wide, wide), wide)
            got = jnp.dot(pick, raw[q, slot, :, cols], preferred_element_type=F32)
            xc[slot * cap:(slot + 1) * cap, cols] = got.astype(BF16)

    gu_t, dn_t, hop, link, lags = cfg["gu_t"], cfg["dn_t"], cfg["hop"], cfg["link"], cfg["lags"]

    def settle(ends, when):
        return next((end for end in ends if end >= when), when)

    def gather_events(q, ends):
        events, queue, free, actions = [], [], {"x": 0.0, "z": 0.0}, {}
        piece = cfg["piece"]
        for p in range(pieces):
            def from_y(p=p):
                y_piece(q, p).wait_recv()
                x_piece(q, p).start()
                z_piece(q, p).start()
                forward(q, 0, p).start()

            def from_x(p=p):
                x_piece(q, p).wait_recv()
                if p % 2 == 1:
                    diagonal(q, p).start()
                forward(q, 1, p).start()

            def from_z(p=p):
                z_piece(q, p).wait_recv()
                if p % 2 == 0:
                    diagonal(q, p).start()
                forward(q, 2, p).start()

            def from_both(p=p):
                diagonal(q, p).wait_recv()
                forward(q, 3, p).start()

            arrive = cfg["late"] + piece * (p + 1)
            events.append((arrive, from_y))
            queue += [(settle(ends, arrive), p, "x", "first"), (settle(ends, arrive), p, "z", "first")]
            actions.update({("x", "first", p): from_x, ("z", "first", p): from_z,
                            ("x", "then", p): from_both, ("z", "then", p): from_both})
        while queue:
            queue.sort()
            issue, p, wire, kind = queue.pop(0)
            free[wire] = max(issue, free[wire]) + piece
            events.append((free[wire] + hop, actions[(wire, kind, p)]))
            if kind == "first" and (p % 2 == 1) == (wire == "x"):
                queue.append((settle(ends, free[wire] + hop), p, "z" if wire == "x" else "x", "then"))
        return events

    def run(actions):
        for action in actions:
            action()

    last = pairs - 1
    ahead_x = min(2, nch)

    for q in range(pairs):
        begin = cfg["gu0"] if q == 0 else cfg["gu1"]
        skip = 2 if q == 0 else 0
        ends = [begin + max(0, j + 1 - skip) * gu_t for j in range(nf)]
        dn_at = ends[-1]
        ends += [dn_at + (j + 1) * dn_t for j in range(nch + 1)]
        events = []
        if q == 0:
            for k in range(1, pairs):
                events += gather_events(k, ends)
        else:
            for c in range(nch):
                at = lags[0] * dn_t + hop + link * (c + 1) + cfg["slack"]
                events.append((at, functools.partial(stage_x, q - 1, c)))
                at = settle(ends, at) + hop + 0.7 * link
                events.append((at, functools.partial(stage_swap, q - 1, c)))
                at = max(settle(ends, at) + hop + link, dn_at + (c - 1.5) * dn_t)
                events.append((at, functools.partial(stage_z, q - 1, c)))
        for c in range(nch):
            events.append((dn_at + (c + lags[min(q, 1)] - 0.5) * dn_t, functools.partial(stage_mate, q, c)))
        if q == last:
            for c in range(ahead_x):
                at = dn_at + lags[1] * dn_t + hop + link * (c + 1) + 1.5
                events.append((at, functools.partial(stage_x, q, c)))
        table = plan(events, ends)

        def gate_up(j, lo, hi):
            slot = j % 2
            gate = jnp.dot(xc[lo:hi], wgu[slot, 0], preferred_element_type=F32)
            up = jnp.dot(xc[lo:hi], wgu[slot, 1], preferred_element_type=F32)
            hidden = (gate * (1.0 / (1.0 + jnp.exp(-gate))) * up).astype(BF16)
            hid[lo:hi, pl.ds(pl.multiple_of(j * ft, ft), ft)] = hidden

        def gu_wait(j):
            for copy in gu_load(j, j % 2):
                copy.wait()

        def gu_refill(j):
            @pl.when(j + 2 < nf)
            def _():
                for copy in gu_load(j + 2, j % 2):
                    copy.start()

        if q == 0:
            compact(0, 0)
            for copy in gu_load(1, 1):
                copy.start()
            greet()

            @pl.loop(0, 2)
            def _(j):
                gu_wait(j)
                gate_up(j, 0, cap)

            routes()
            compact(0, 1)

            @pl.loop(0, 2)
            def _(j):
                gate_up(j, cap, 2 * cap)
                gu_refill(j)

            run(table[0])
            run(table[1])
        else:
            for slot in range(2):
                compact(q, slot)

        @pl.loop(skip, nf)
        def _(j):
            gu_wait(j)
            gate_up(j, 0, 2 * cap)
            gu_refill(j)
            for step in range(skip, nf):
                if table[step]:
                    pl.when(j == step)(functools.partial(run, table[step]))

        def expand():
            return [jnp.dot(emat[i], ys[i], preferred_element_type=F32).astype(BF16).reshape(nz1, 2, 2, owned, cw)
                    for i in range(2)]

        def put(c, values):
            keep[q, c], give[c] = values
            d2d(q, c).start()

        def project(slot):
            y = jnp.dot(hid[...], wdn[slot], preferred_element_type=F32)
            ys[0] = (y[:cap] * wcol[0, :, :1]).astype(BF16)
            ys[1] = (y[cap:] * wcol[1, :, :1]).astype(BF16)

        def refill(c, slot):
            ahead = c + slots
            if q + 1 < pairs:
                dn_load(ahead % nch, slot).start()
            else:
                @pl.when(ahead < nch)
                def _():
                    dn_load(ahead, slot).start()

        dn_load(0, 0).wait()
        project(0)
        refill(0, 0)
        run(table[nf])

        @pl.loop(1, nch)
        def _(c):
            slot = c % slots
            dn_load(c, slot).wait()
            if q > 0:
                d2d(q - 1, c - 1).wait_send()
            values = expand()
            keep[q, c - 1], give[c - 1] = values
            project(slot)
            d2d(q, c - 1).start()
            refill(c, slot)
            if q + 1 < pairs:
                for i in range(2):
                    for k, copy in enumerate(gu_load(i, i)):
                        pl.when(c == min(nch - 1, 1 + 2 * (2 * i + k)))(lambda copy=copy: copy.start())

            for step in range(1, nch):
                if table[nf + step]:
                    pl.when(c == step)(functools.partial(run, table[nf + step]))

        if q > 0:
            d2d(q - 1, nch - 1).wait_send()
        put(nch - 1, expand())
        run(table[nf + nch])
        run(table[nf + nch + 1])

    def sent(q, c):
        if q == last:
            d2d(q, c).wait_send()
        xsend(q, c).wait_send()
        zswap(q, c).wait_send()
        if q == 0:
            zall(q, c).wait_send()
        else:
            ysend(q, c).wait_send()

    def sent_tokens():
        mate_tokens().wait_send()
        for k in range(1, experts):
            route_copy(k).wait_send()
        for q in range(1, pairs):
            for p in range(pieces):
                for copy in (y_piece, x_piece, z_piece, diagonal):
                    copy(q, p).wait_send()
                for kind in range(4):
                    forward(q, kind, p).wait_send()

    @pl.loop(ahead_x, nch)
    def _(n):
        stage_x(last, n)

        @pl.when(n >= 2)
        def _():
            stage_swap(last, n - 2)

        @pl.when(n >= 5)
        def _():
            stage_z(last, n - 5)

        @pl.when(n >= 7)
        def _():
            stage_y(n - 7)

        for q in range(last):
            sent(q, n)
        pl.when(n == max(ahead_x, nch // 2))(sent_tokens)

    @pl.loop(max(0, nch - 2), nch)
    def _(n):
        stage_swap(last, n)

    @pl.loop(max(0, nch - 5), nch)
    def _(n):
        stage_z(last, n)

    @pl.loop(max(0, nch - 7), nch)
    def _(n):
        stage_y(n)

    for c in range(ahead_x):
        for q in range(last):
            sent(q, c)

    @pl.loop(0, nch)
    def _(c):
        sent(last, c)


def body(tokens, expert_ids, gate_weights, w_gate, w_up, w_down):
    rows, width = tokens.shape
    experts = lax.axis_size("expert")
    parts = lax.axis_size("tensor")
    ff = w_gate.shape[2]
    cap = rows * 3 // 4
    pairs, nz, owned = experts // 2, parts // 2, rows // parts
    ft, cw, pieces, slots = 256, 512, 4, 3
    nch = width // cw
    others = pairs - 1

    hot = expert_ids[None, :, :] == jnp.arange(experts, dtype=jnp.int32)[:, None, None]
    weight = jnp.sum(jnp.where(hot, gate_weights[None], 0.0), axis=2)
    weight = jnp.broadcast_to(weight[:, None, :], (experts, 8, rows))

    cfg = dict(
        dims=(experts, parts, rows, cap, width, ff), ft=ft, cw=cw, pieces=pieces, slots=slots,
        gu_t=2.7, dn_t=1.2, hop=1.9, link=2.85, lags=(8.0, 3.0), piece=4.3, gu0=9.8, gu1=20.0, late=3.0, slack=2.5,
    )
    dma = pltpu.SemaphoreType.DMA
    any_space = pl.BlockSpec(memory_space=pl.ANY)
    vmem = pl.BlockSpec(memory_space=pltpu.VMEM)
    return pl.pallas_call(
        functools.partial(moe_kernel, cfg),
        out_shape=jax.ShapeDtypeStruct((owned, width), BF16),
        in_specs=[any_space, vmem, any_space, any_space, any_space],
        out_specs=vmem,
        scratch_shapes=[
            pltpu.VMEM((pairs, 2, rows, width), BF16),
            pltpu.VMEM((2 * cap, width), BF16),
            pltpu.VMEM((2 * cap, ff), BF16),
            pltpu.VMEM((2, 2, width, ft), BF16),
            pltpu.VMEM((slots, ff, cw), BF16),
            pltpu.VMEM((2, cap, cw), BF16),
            pltpu.VMEM((pairs, nch, nz // 2, 2, 2, owned, cw), BF16),
            pltpu.VMEM((nch, nz // 2, 2, 2, owned, cw), BF16),
            pltpu.VMEM((pairs, nch, nz // 2, 2, 2, owned, cw), BF16),
            pltpu.VMEM((pairs, nch, nz // 2, 2, owned, cw), BF16),
            pltpu.VMEM((pairs, nch, nz // 2, owned, cw), BF16),
            pltpu.VMEM((pairs, nch, nz // 2 - 1, owned, cw), BF16),
            pltpu.VMEM((others, nch, owned, cw), BF16),
            pltpu.VMEM((nch, owned, cw), F32),
            pltpu.VMEM((experts, 8, rows), F32),
            pltpu.VMEM((2, rows, cap), BF16),
            pltpu.VMEM((2, cap, 128), F32),
            dma,
            dma((2, 2)),
            dma((slots,)),
            dma((2, experts - 1)),
            dma((2,)),
            dma((2, others, pieces)),
            dma((2, others, pieces)),
            dma((2, others, pieces)),
            dma((2, others, pieces)),
            dma((2, others, 4 * pieces)),
            dma((2, pairs, nch)),
            dma((2, pairs, nch)),
            dma((2, pairs, nch)),
            dma((2, pairs, nch)),
            dma((2, others, nch)),
        ],
        compiler_params=pltpu.CompilerParams(
            collective_id=0, has_side_effects=True, vmem_limit_bytes=67043328),
    )(tokens, weight, w_gate[0], w_up[0], w_down[0])


def solution(mesh):
    placed = (
        P("expert", None),
        P("expert", None),
        P("expert", None),
        P("expert", None, "tensor"),
        P("expert", None, "tensor"),
        P("expert", "tensor", None),
    )
    return jax.shard_map(
        body, mesh=mesh, in_specs=placed, out_specs=P(("expert", "tensor"), None), check_vma=False
    )
```
